32 devices in a mesh: grp: 2 (over y), blk: 16 (over z, x, core).
Axes of the slice: x: 2, y: 2, z: 4, core: 2. Of those that a mesh axis runs over, the one named last changes fastest.
Arguments:
- queries: bfloat16 [2048, 4096], P('blk'), may hold values from -15 to 15
- cache_keys: bfloat16 [1024, 512], P(('grp', 'blk')), may hold values from -5 to 5
- cache_values: bfloat16 [1024, 512], P(('grp', 'blk')), may hold values from -6 to 6
- new_keys: bfloat16 [2048, 512], P('blk'), may hold values from -6 to 6
- new_values: bfloat16 [2048, 512], P('blk'), may hold values from -6 to 6
- prefix_length: int32 [1], replicated, may hold values from 512 to 1024
- token_order: int32 [2048], P('blk'), may hold values from 0 to 2047, as said below
Outputs:
- attended: bfloat16 [2048, 4096], P('blk', 'grp')
The draws below stay inside these ranges and needn't reach their ends.
Inputs may be any that keep to these rules, and one draw needn't show every extreme that they name: Cache slots from prefix_length[0] on are unused. `token_order`: a permutation of 0 to 2047 made of runs of 64 consecutive values, each run starting at a multiple of 64.
All inputs are finite; a program needn't handle non-finite values.
Results may differ from the reference program's by a relative error of at most 0.0044.
Values may be sent and summed in bfloat16 or wider, within the bound.
A program may use at most 64 MiB of HBM per device.

```python
import jax
import jax.numpy as jnp
from jax import lax

HQ = 32
KVH = 4
HD = 128
TOK_DEV = 128
NEW = 2048
KEYS = 1024


def draw_queries(key, part):
    normal_part = jax.random.normal(key, (NEW, HQ * HD), jnp.float32)
    return jnp.clip(3.0 * normal_part, -15.0, 15.0).astype(jnp.bfloat16)


def draw_cache_keys(key, part):
    normal_part = jax.random.normal(key, (KEYS, KVH * HD), jnp.float32)
    return jnp.clip(normal_part, -5.0, 5.0).astype(jnp.bfloat16)


def draw_token_order(key, part):
    run_length = TOK_DEV // 2
    run_count = NEW // run_length
    order_runs = jax.random.permutation(key, run_count).astype(jnp.int32)
    within_run = jnp.arange(run_length, dtype=jnp.int32)
    return (order_runs[:, None] * run_length + within_run[None, :]).reshape(NEW).astype(jnp.int32)


def block_scale(own_key, dims, cuts, low, largest):
    def one(axis_at, shards_of):
        steps = jax.random.uniform(jax.random.fold_in(jax.random.fold_in(own_key, 6), axis_at), (shards_of,), jnp.float32, low / len(cuts), largest / len(cuts))
        return jnp.repeat(jnp.exp(steps), dims[axis_at] // shards_of).reshape((-1,) + (1,) * (len(dims) - axis_at - 1))

    factor_of = one(*cuts[0])
    for cut in cuts[1:]:
        factor_of = factor_of * one(*cut)
    return factor_of


def centred(stream_key, dims, deviation, limit, shards=(), held_as=jnp.bfloat16):
    entries = deviation * jax.random.normal(stream_key, dims, jnp.float32)
    if shards:
        entries = entries * block_scale(stream_key, dims, shards, -0.22, 0.18)
    return jnp.clip(entries, -limit, limit).astype(held_as)


def setup_inputs(seed: int = 0) -> dict:
    keys = jax.random.split(jax.random.key(seed), 8)
    return {
        "queries": draw_queries(jax.random.fold_in(keys[7], 71), 0),
        "cache_keys": draw_cache_keys(jax.random.fold_in(keys[7], 71), 0),
        "cache_values": centred(keys[2], (KEYS, KVH * HD), 1.0, 6.0, ((0, 32),)),
        "new_keys": centred(keys[3], (NEW, KVH * HD), 1.0, 6.0, ((0, 16),)),
        "new_values": centred(keys[4], (NEW, KVH * HD), 1.0, 6.0, ((0, 16),)),
        "prefix_length": jax.random.randint(keys[5], (1,), KEYS // 2, KEYS + 1).astype(jnp.int32),
        "token_order": draw_token_order(jax.random.fold_in(keys[7], 71), 0),
    }


def reference(queries, cache_keys, cache_values, new_keys, new_values, prefix_length, token_order):
    all_keys = jnp.concatenate([cache_keys, new_keys], axis=0)
    all_values = jnp.concatenate([cache_values, new_values], axis=0)
    slot_ids = jnp.arange(KEYS, dtype=jnp.int32)
    cache_open = jnp.broadcast_to((slot_ids < prefix_length[0])[None, :], (NEW, KEYS))
    causal_open = token_order[None, :] <= token_order[:, None]
    visible = jnp.concatenate([cache_open, causal_open], axis=1)
    group_size = HQ // KVH
    score_scale = HD ** -0.5

    def one_head(head_id):
        kv_head = head_id // group_size
        head_query = lax.dynamic_slice_in_dim(queries, head_id * HD, HD, 1)
        head_keys = lax.dynamic_slice_in_dim(all_keys, kv_head * HD, HD, 1)
        head_values = lax.dynamic_slice_in_dim(all_values, kv_head * HD, HD, 1)
        scores = jnp.dot(head_query, head_keys.T, preferred_element_type=jnp.float32) * score_scale
        scores = jnp.where(visible, scores, -1.0e30)
        row_max = jnp.max(scores, axis=1, keepdims=True)
        weights = jnp.where(visible, jnp.exp(scores - row_max), 0.0)
        row_total = jnp.sum(weights, axis=1, keepdims=True)
        result = jnp.dot(weights.astype(jnp.bfloat16), head_values, preferred_element_type=jnp.float32) / row_total
        return result.astype(jnp.bfloat16)

    per_head = lax.map(one_head, jnp.arange(HQ, dtype=jnp.int32))
    return per_head.transpose(1, 0, 2).reshape(NEW, HQ * HD)
```

```python
import functools
import math

import jax
import jax.numpy as jnp
from jax import lax
from jax.experimental import pallas as pl
from jax.experimental.pallas import tpu as pltpu
from jax.sharding import PartitionSpec as P

HQ = 32
KVH = 4
HD = 128
MESH = pl.DeviceIdType.MESH
MASKED = -1e30
TILES = 1

def nearest_first(z_count):
    return [sorted(range(z_count), key=lambda other: (abs(other - z), abs(2 * other - z_count + 1))) for z in range(z_count)]

def pick(z, column):
    value = jnp.int32(column[0])
    for at in range(1, len(column)):
        value = jnp.where(z == at, jnp.int32(column[at]), value)
    return value

def kernel(
    groups, blocks,
    q_hbm, ck_hbm, cv_hbm, nk_hbm, nv_hbm, prefix_ref, order_hbm,
    out_ref,
    nbuf, cbuf, obuf, stage, qraw, qs, order_q, m_s, l_s, acc_s,
    load_sem, y_send, y_recv,
    up_send, down_send, x_send, sib_send, sibx_send,
    z_recv, x_recv, sib_recv, sibx_recv,
):
    heads = HQ // groups
    group_size = HQ // KVH
    kv_count = max(1, heads // group_size)
    sub_heads = heads // kv_count
    cols = kv_count * HD
    tok = nbuf.shape[1]
    slots = ck_hbm.shape[0]
    z_count = blocks // 4
    rows = sub_heads * tok

    g = lax.axis_index("grp")
    me = lax.axis_index("blk")
    z = me // 4
    x = (me // 2) % 2
    c = me % 2

    def block_of(zz, xx, cc):
        return (zz * 2 + xx) * 2 + cc

    sibling = block_of(z, x, 1 - c)
    across = block_of(z, 1 - x, c)
    has_up = z < z_count - 1
    has_down = z > 0
    middle = jnp.logical_and(has_up, has_down)

    def head_cols(group):
        return pl.ds(pl.multiple_of((group * heads // group_size) * HD, HD), cols)

    loads = [
        pltpu.make_async_copy(nk_hbm.at[:, head_cols(g)], nbuf.at[me, :, pl.ds(0, cols)], load_sem.at[0]),
        pltpu.make_async_copy(nv_hbm.at[:, head_cols(g)], nbuf.at[me, :, pl.ds(cols, cols)], load_sem.at[1]),
        pltpu.make_async_copy(order_hbm, obuf.at[me], load_sem.at[2]),
        pltpu.make_async_copy(ck_hbm, stage.at[0], load_sem.at[3]),
        pltpu.make_async_copy(cv_hbm, stage.at[1], load_sem.at[4]),
        pltpu.make_async_copy(ck_hbm.at[:, head_cols(g)], cbuf.at[me, pl.ds(g * slots, slots), pl.ds(0, cols)], load_sem.at[5]),
        pltpu.make_async_copy(cv_hbm.at[:, head_cols(g)], cbuf.at[me, pl.ds(g * slots, slots), pl.ds(cols, cols)], load_sem.at[6]),
        pltpu.make_async_copy(q_hbm.at[:, pl.ds(pl.multiple_of(g * heads * HD, HD), heads * HD)], qraw, load_sem.at[7]),
    ]

    for load in loads:
        load.start()

    barrier = pltpu.get_barrier_semaphore()

    def greet(group, block):
        pl.semaphore_signal(barrier, inc=1, device_id=(group, block), device_id_type=MESH)

    greet(g, sibling)
    greet(g, across)
    for step in range(1, groups):
        greet((g + step) % groups, me)
    pl.when(has_up)(lambda: greet(g, me + 4))
    pl.when(has_down)(lambda: greet(g, me - 4))
    pl.semaphore_wait(barrier, 1 + groups + jnp.where(has_up, 1, 0) + jnp.where(has_down, 1, 0))

    bufs = (nbuf, obuf, cbuf)

    def remote(kind, block, target, send, recv, at):
        ref = bufs[kind].at[block]
        return pltpu.make_async_remote_copy(
            src_ref=ref, dst_ref=ref, send_sem=send.at[kind, at], recv_sem=recv.at[kind, at],
            device_id=(g, target), device_id_type=MESH,
        )

    def send_up(kind, zz):
        return remote(kind, block_of(zz, x, c), me + 4, up_send, z_recv, zz)

    def send_down(kind, zz):
        return remote(kind, block_of(zz, x, c), me - 4, down_send, z_recv, zz)

    def send_x(kind, zz):
        return remote(kind, block_of(zz, x, c), across, x_send, x_recv, zz)

    def send_sib(kind, zz):
        return remote(kind, block_of(zz, x, c), sibling, sib_send, sib_recv, zz)

    def send_sibx(kind, zz):
        return remote(kind, block_of(zz, 1 - x, c), sibling, sibx_send, sibx_recv, zz)

    for load in loads[3:5]:
        load.wait()
    swaps = []
    for step in range(1, groups):
        other = (g + step) % groups
        for part in range(2):
            swaps.append(pltpu.make_async_remote_copy(
                src_ref=stage.at[part, :, head_cols(other)],
                dst_ref=cbuf.at[me, pl.ds(g * slots, slots), pl.ds(part * cols, cols)],
                send_sem=y_send.at[step, part], recv_sem=y_recv.at[step, part],
                device_id=(other, me), device_id_type=MESH,
            ))
    for swap in swaps:
        swap.start()

    def launch_own(kind):
        pl.when(has_up)(lambda: send_up(kind, z).start())
        pl.when(has_down)(lambda: send_down(kind, z).start())
        send_x(kind, z).start()
        send_sib(kind, z).start()

    for load in loads[:3]:
        load.wait()
    launch_own(0)
    launch_own(1)
    for load in loads[5:7]:
        load.wait()

    loads[7].wait()
    factor = HD ** -0.5 * math.log2(math.e)
    for head in range(heads):
        scaled = qraw[:, head * HD:(head + 1) * HD].astype(jnp.float32) * factor
        high = scaled.astype(jnp.bfloat16)
        low = (scaled - high.astype(jnp.float32)).astype(jnp.bfloat16)
        kv, sub = head // sub_heads, head % sub_heads
        qs[kv, sub * tok:(sub + 1) * tok, 0:HD] = high
        qs[kv, sub * tok:(sub + 1) * tok, HD:2 * HD] = low
    order_q[...] = jnp.broadcast_to(obuf[me].astype(jnp.float32), (tok, tok)).T

    for swap in swaps:
        swap.wait_recv()
    launch_own(2)

    prefix = prefix_ref[0]

    def attend(zz, xx, first=False):
        block = block_of(zz, xx, 0)
        cache_rows = cbuf.shape[1]
        lane = lax.broadcasted_iota(jnp.int32, (1, 2 * cache_rows), 1)
        within = lane % cache_rows
        slot = (within // slots) * (slots * blocks) + (block + lane // cache_rows) * slots + within % slots
        cache_bias = jnp.where(slot < prefix, 0.0, MASKED).astype(jnp.float32)
        pieces = [
            jnp.where(obuf[block + at].astype(jnp.float32) <= order_q[...], 0.0, MASKED) for at in range(2)
        ] + [jnp.broadcast_to(cache_bias, (tok, 2 * cache_rows))]
        bias = jnp.concatenate(pieces, axis=1)
        keys_n = 2 * (tok + cache_rows)
        rows = sub_heads * tok

        def gathered(at):
            return jnp.concatenate(
                [nbuf[block, :, at], nbuf[block + 1, :, at], cbuf[block, :, at], cbuf[block + 1, :, at]], axis=0
            )

        def operands(kv):
            keys = gathered(slice(kv * HD, (kv + 1) * HD))
            values = gathered(slice(cols + kv * HD, cols + (kv + 1) * HD))
            ones = jnp.ones((keys_n, HD), jnp.bfloat16)
            return jnp.concatenate([keys, keys], axis=1), jnp.concatenate([values, ones], axis=1)

        heads_tile = max(1, sub_heads // TILES)
        rows = heads_tile * tok
        pairs = [operands(kv) for kv in range(kv_count)]
        tiles = [(kv, sub) for kv in range(kv_count) for sub in range(0, sub_heads, heads_tile)]

        def score(kv, sub):
            at = slice(sub * tok, sub * tok + rows)
            return lax.dot_general(
                qs[kv, at], pairs[kv][0], (((1,), (1,)), ((), ())), preferred_element_type=jnp.float32
            )

        ahead = score(*tiles[0])
        for index, (kv, sub) in enumerate(tiles):
            s = ahead
            if index + 1 < len(tiles):
                ahead = score(*tiles[index + 1])
            at = slice(sub * tok, sub * tok + rows)
            s = (s.reshape(heads_tile, tok, keys_n) + bias[None]).reshape(rows, keys_n)
            chunks = [s[:, lanes:lanes + HD] for lanes in range(0, keys_n, HD)]
            peak = jnp.max(functools.reduce(jnp.maximum, chunks), axis=1, keepdims=True)
            if first:
                new_max = jnp.broadcast_to(peak, (rows, HD))
            else:
                old_max = m_s[kv, at]
                new_max = jnp.maximum(old_max, peak)
            p = jnp.concatenate([jnp.exp2(chunk - new_max).astype(jnp.bfloat16) for chunk in chunks], axis=1)
            o = jnp.dot(p, pairs[kv][1], preferred_element_type=jnp.float32)
            m_s[kv, at] = new_max
            if first:
                l_s[kv, at] = o[:, HD:]
                acc_s[kv, at] = o[:, :HD]
            else:
                alpha = jnp.exp2(old_max - new_max)
                l_s[kv, at] = l_s[kv, at] * alpha + o[:, HD:]
                acc_s[kv, at] = acc_s[kv, at] * alpha + o[:, :HD]

    def arrive_z(zz):
        for kind in range(3):
            remote(kind, block_of(zz, x, c), across, x_send, z_recv, zz).wait_recv()
            pl.when(jnp.logical_and(zz < z, has_up))(lambda: send_up(kind, zz).start())
            pl.when(jnp.logical_and(zz > z, has_down))(lambda: send_down(kind, zz).start())
            send_x(kind, zz).start()
            send_sib(kind, zz).start()

    def arrive_x(zz):
        for kind in range(3):
            remote(kind, block_of(zz, 1 - x, c), across, x_send, x_recv, zz).wait_recv()
            send_sibx(kind, zz).start()

    def own_column(zz, first=False):
        for kind in range(3):
            remote(kind, block_of(zz, x, 1 - c), sibling, sib_send, sib_recv, zz).wait_recv()
        attend(zz, x, first)

    def other_column(zz):
        for kind in range(3):
            remote(kind, block_of(zz, 1 - x, 1 - c), sibling, sibx_send, sibx_recv, zz).wait_recv()
        attend(zz, 1 - x)

    table = nearest_first(z_count)
    zs = [pick(z, [table[at][step] for at in range(z_count)]) for step in range(z_count)]

    own_column(z, first=True)
    for step in range(1, z_count):
        if step == 1:
            arrive_z(zs[1])
        else:
            pl.when(jnp.logical_not(middle))(lambda: arrive_z(zs[step]))
        if step + 1 < z_count:
            pl.when(middle)(lambda: arrive_z(zs[step + 1]))
        arrive_x(zs[step - 1])
        own_column(zs[step])
        other_column(zs[step - 1])
    last = zs[z_count - 1]
    arrive_x(last)
    other_column(last)

    for head in range(heads):
        kv, sub = head // sub_heads, head % sub_heads
        at = slice(sub * tok, (sub + 1) * tok)
        out_ref[:, head * HD:(head + 1) * HD] = (acc_s[kv, at] / l_s[kv, at]).astype(out_ref.dtype)

    for swap in swaps:
        swap.wait_send()
    for kind in range(3):
        pl.when(has_up)(lambda: send_up(kind, z).wait_send())
        pl.when(has_down)(lambda: send_down(kind, z).wait_send())
        for zz in range(z_count):
            pl.when(jnp.logical_and(zz < z, has_up))(lambda: send_up(kind, zz).wait_send())
            pl.when(jnp.logical_and(zz > z, has_down))(lambda: send_down(kind, zz).wait_send())
            send_x(kind, zz).wait_send()
            send_sib(kind, zz).wait_send()
            send_sibx(kind, zz).wait_send()

def in_hbm(array):
    return pltpu.with_memory_space_constraint(array, pltpu.HBM)


def solution(mesh):
    groups = mesh.shape["grp"]
    blocks = mesh.shape["blk"]

    def on_device(queries, cache_keys, cache_values, new_keys, new_values, prefix_length, token_order):
        tok = queries.shape[0]
        slots = cache_keys.shape[0]
        heads = HQ // groups
        kv_count = max(1, heads // (HQ // KVH))
        cols = kv_count * HD
        rows = heads // kv_count * tok
        z_count = blocks // 4
        dma = pltpu.SemaphoreType.DMA
        hbm = pl.BlockSpec(memory_space=pltpu.HBM)
        return pl.pallas_call(
            functools.partial(kernel, groups, blocks),
            out_shape=jax.ShapeDtypeStruct((tok, heads * HD), jnp.bfloat16),
            in_specs=[hbm] * 5 + [pl.BlockSpec(memory_space=pltpu.SMEM), hbm],
            out_specs=pl.BlockSpec(memory_space=pltpu.VMEM),
            scratch_shapes=[
                pltpu.VMEM((blocks, tok, 2 * cols), jnp.bfloat16),
                pltpu.VMEM((blocks, groups * slots, 2 * cols), jnp.bfloat16),
                pltpu.VMEM((blocks, 1, tok), jnp.int32),
                pltpu.VMEM((2, slots, KVH * HD), jnp.bfloat16),
                pltpu.VMEM((tok, heads * HD), jnp.bfloat16),
                pltpu.VMEM((kv_count, rows, 2 * HD), jnp.bfloat16),
                pltpu.VMEM((tok, tok), jnp.float32),
                pltpu.VMEM((kv_count, rows, HD), jnp.float32),
                pltpu.VMEM((kv_count, rows, HD), jnp.float32),
                pltpu.VMEM((kv_count, rows, HD), jnp.float32),
                dma((8,)), dma((groups, 2)), dma((groups, 2)),
                dma((3, z_count)), dma((3, z_count)), dma((3, z_count)), dma((3, z_count)), dma((3, z_count)),
                dma((3, z_count)), dma((3, z_count)), dma((3, z_count)), dma((3, z_count)),
            ],
            compiler_params=pltpu.CompilerParams(
                collective_id=0, has_side_effects=True, vmem_limit_bytes=28 * 1024 * 1024
            ),
        )(
            *[in_hbm(a) for a in (queries, cache_keys, cache_values, new_keys, new_values)],
            prefix_length, in_hbm(token_order.reshape(1, tok)),
        )

    placed = (
        P("blk", None), P(("grp", "blk"), None), P(("grp", "blk"), None),
        P("blk", None), P("blk", None), P(), P("blk"),
    )
    return jax.shard_map(on_device, mesh=mesh, in_specs=placed, out_specs=P("blk", "grp"), check_vma=False)
```
